128 devices in a mesh: row: 8 (over z, core), col: 16 (over y, x).
Axes of the slice: x: 4, y: 4, z: 4, core: 2. Of those that a mesh axis runs over, the one named last changes fastest.
Arguments:
- src_field: bfloat16 [64, 4194304], P(None, ('row', 'col')), may hold values from 0.5 to 2
- src_area: float32 [4194304], P(('row', 'col')), may hold values from 0.3 to 3
- tgt_area: float32 [1048576], P(('row', 'col')), may hold values from 0.3 to 3
- weights: bfloat16 [49152, 128, 128], P(('row', 'col')), may hold values from 0 to 0.0025939941
- send_index: int32 [128, 128, 2], P(('row', 'col')), may hold values from -1 to 255, as said below
- pair_slot: int32 [49152], P(('row', 'col')), may hold values from 0 to 255, as said below
- pair_target: int32 [49152], P(('row', 'col')), may hold values from 0 to 63, as said below
Outputs:
- target_field: float32 [64, 1048576], P(None, ('row', 'col'))
The draws below stay inside these ranges and needn't reach their ends.
Inputs may be any that keep to these rules, and one draw needn't show every extreme that they name: `send_index`: in each [s, r] the live entries (not -1) come first and there are 1 to 2 of them; every sender sends to every receiver; for each receiver some sender fills all 2 slots. `pair_slot`: each pair of device r names a live slot of what device r receives; every live slot is named by some pair of device r. `pair_target`: every local target block of a device is named by some pair of that device.
All inputs are finite; a program needn't handle non-finite values.
Results may differ from the reference program's by a relative error of at most 0.0003.
Values may be sent and summed in bfloat16 or wider, within the bound.
A program may use at most 128 MiB of HBM per device.

```python
import math
import jax
import jax.numpy as jnp
from jax import lax

VARS = 8
LEV = 8
BLK = 128
CAP = 2
SB_DEV = 256
TB_DEV = 64
PAIRS_DEV = 384
NEAR = 128
NSB = 32768
NTB = 8192
PAIRS = 49152
N_ROW = 8
N_COL = 16


def routing(key):
    peer_count = N_ROW * N_COL
    base = jax.random.fold_in(key, 7)
    offsets = jnp.arange(NEAR, dtype=jnp.int32)
    receivers = jnp.arange(peer_count, dtype=jnp.int32)
    senders_of = (receivers[:, None] + offsets[None, :]) % peer_count
    near_counts = jax.random.randint(jax.random.fold_in(base, 1), (peer_count, NEAR), 1, CAP + 1)
    full_near = jax.random.randint(jax.random.fold_in(base, 2), (peer_count,), 0, NEAR)
    near_counts = jnp.where(jnp.arange(NEAR)[None, :] == full_near[:, None], CAP, near_counts)
    receiver_grid = jnp.broadcast_to(receivers[:, None], (peer_count, NEAR))
    counts = jnp.zeros((peer_count, peer_count), jnp.int32).at[senders_of, receiver_grid].set(near_counts)
    local_pick = jax.random.randint(jax.random.fold_in(base, 3), (peer_count, peer_count, CAP), 0, SB_DEV)
    alive_mask = jnp.arange(CAP)[None, None, :] < counts[:, :, None]
    send_index = jnp.where(alive_mask, local_pick, -1).astype(jnp.int32)
    position = jnp.arange(PAIRS_DEV, dtype=jnp.int32)
    near_pos = jnp.minimum(position // CAP, NEAR - 1)
    slot_pos = position % CAP
    first_sender = senders_of[:, near_pos]
    first_count = near_counts[:, near_pos]
    first_pick = jnp.where(slot_pos[None, :] < first_count, first_sender * CAP + slot_pos[None, :], first_sender * CAP)
    extra_near = jax.random.randint(jax.random.fold_in(base, 4), (peer_count, PAIRS_DEV), 0, NEAR)
    extra_raw = jax.random.randint(jax.random.fold_in(base, 6), (peer_count, PAIRS_DEV), 0, CAP)
    extra_sender = jnp.take_along_axis(senders_of, extra_near, axis=1)
    extra_count = jnp.take_along_axis(near_counts, extra_near, axis=1)
    extra_pick = extra_sender * CAP + extra_raw % extra_count
    slots_all = jnp.where((position < NEAR * CAP)[None, :], first_pick, extra_pick)
    targets_all = jnp.broadcast_to((position % TB_DEV)[None, :], (peer_count, PAIRS_DEV))
    shuffle = jax.vmap(lambda sub: jax.random.permutation(sub, PAIRS_DEV))(jax.random.split(jax.random.fold_in(base, 5), peer_count))
    pair_slot = jnp.take_along_axis(slots_all, shuffle, axis=1).reshape(-1).astype(jnp.int32)
    pair_target = jnp.take_along_axis(targets_all, shuffle, axis=1).reshape(-1).astype(jnp.int32)
    return (send_index, pair_slot, pair_target)


def draw_send_index(key, part):
    return routing(key)[0]


def draw_pair_slot(key, part):
    return routing(key)[1]


def draw_pair_target(key, part):
    return routing(key)[2]


def shard_levels(stream_key, dims, cuts, smallest, largest):
    def one(dim, blocks):
        heights = jax.random.uniform(jax.random.fold_in(jax.random.fold_in(stream_key, 6), dim), (blocks,), jnp.float32, smallest / len(cuts), largest / len(cuts))
        return jnp.repeat(jnp.exp(heights), dims[dim] // blocks).reshape((-1,) + (1,) * (len(dims) - dim - 1))

    gain = one(*cuts[0])
    for cut in cuts[1:]:
        gain = gain * one(*cut)
    return gain


def setup_inputs(seed: int = 0) -> dict:
    splits = jax.random.split(jax.random.key(seed), 8)
    src_field = jnp.clip(0.5 + 1.5 * jax.random.uniform(splits[0], (VARS * LEV, NSB * BLK), jnp.float32) ** shard_levels(splits[0], (VARS * LEV, NSB * BLK), ((1, 128),), -0.2, 0.2), 0.5, 2.0).astype(jnp.bfloat16)
    src_area = jnp.clip(jnp.exp(math.log(3.0) - 2.3025851 * jax.random.uniform(splits[1], (NSB * BLK,), jnp.float32) ** shard_levels(splits[1], (NSB * BLK,), ((0, 128),), -0.2, 0.2)), 0.3, 3.0)
    tgt_area = jnp.clip(jnp.exp(math.log(3.0) - 2.3025851 * jax.random.uniform(splits[2], (NTB * BLK,), jnp.float32) ** shard_levels(splits[2], (NTB * BLK,), ((0, 128),), -0.2, 0.2)), 0.3, 3.0)
    weights = jnp.clip(0.0025939941 * jax.random.uniform(splits[3], (PAIRS, BLK, BLK), jnp.float32) ** shard_levels(splits[3], (PAIRS, BLK, BLK), ((0, 128),), -0.2, 0.2), 0.0, 0.0025939941).astype(jnp.bfloat16)
    send_index = draw_send_index(jax.random.fold_in(splits[7], 71), 0)
    pair_slot = draw_pair_slot(jax.random.fold_in(splits[7], 71), 0)
    pair_target = draw_pair_target(jax.random.fold_in(splits[7], 71), 0)
    return {"src_field": src_field, "src_area": src_area, "tgt_area": tgt_area, "weights": weights, "send_index": send_index, "pair_slot": pair_slot, "pair_target": pair_target}


def reference(src_field, src_area, tgt_area, weights, send_index, pair_slot, pair_target):
    peer_count = N_ROW * N_COL
    columns = VARS * LEV
    blocks = src_field.reshape(columns, peer_count * SB_DEV, BLK)

    def per_receiver(receiver):
        slot_ids = lax.dynamic_slice_in_dim(pair_slot, receiver * PAIRS_DEV, PAIRS_DEV)
        targets = lax.dynamic_slice_in_dim(pair_target, receiver * PAIRS_DEV, PAIRS_DEV)
        tiles = lax.dynamic_slice_in_dim(weights, receiver * PAIRS_DEV, PAIRS_DEV, 0)
        sender = slot_ids // CAP
        slot_pos = slot_ids % CAP
        local_ids = send_index[sender, receiver, slot_pos]
        global_ids = (sender * SB_DEV + local_ids).astype(jnp.int32)
        picked = jnp.take(blocks, global_ids, axis=1)
        products = jnp.einsum('cps,pst->pct', picked.astype(jnp.float32), tiles.astype(jnp.float32), precision=lax.Precision.HIGHEST)
        return jax.ops.segment_sum(products, targets, num_segments=TB_DEV)

    regridded = lax.map(per_receiver, jnp.arange(peer_count, dtype=jnp.int32))
    regridded = jnp.transpose(regridded, (2, 0, 1, 3)).reshape(columns, peer_count * TB_DEV * BLK)
    source_mass = jnp.sum(src_field.astype(jnp.float32) * src_area[None, :], axis=1)
    target_mass = jnp.sum(regridded * tgt_area[None, :], axis=1)
    return regridded * (source_mass / target_mass)[:, None]
```

```python
import functools

import jax
import jax.numpy as jnp
from jax import lax
from jax.experimental import pallas as pl
from jax.experimental.pallas import tpu as pltpu
from jax.sharding import Mesh
from jax.sharding import PartitionSpec as P

AXES = ("z", "core", "y", "x")
SIZES = (4, 2, 4, 4)
BLOCK = 128
GATHERED = 16
PAIRS = 32


def collect(index_ref, source_ref, out_ref):
    first = pl.program_id(0) * GATHERED
    for i in range(GATHERED):
        block = jnp.maximum(index_ref[0, i % 2, first // 2 + i // 2], 0)
        columns = pl.ds(pl.multiple_of(block * BLOCK, BLOCK), BLOCK)
        out_ref[i] = source_ref[:, columns]


def outbound_blocks(send_index, source):
    rows, cells = source.shape
    peers, capacity = send_index.shape[1:]
    slots = peers * capacity
    return pl.pallas_call(
        collect,
        out_shape=jax.ShapeDtypeStruct((slots, rows, BLOCK), source.dtype),
        grid_spec=pltpu.PrefetchScalarGridSpec(
            num_scalar_prefetch=1,
            grid=(slots // GATHERED,),
            in_specs=[pl.BlockSpec((rows, cells), lambda i, s: (0, 0))],
            out_specs=pl.BlockSpec((GATHERED, rows, BLOCK), lambda i, s: (i, 0, 0)),
        ),
    )(jnp.swapaxes(send_index, 1, 2), source)


def as_lanes(column):
    rows = column.shape[0]
    wide = jnp.broadcast_to(column, (rows, BLOCK))
    return jnp.transpose(wide)[0:1, :]


def regrid(slot_ref, target_ref, source_ref, weight_ref, area_ref, out_ref, mass_ref):
    step = pl.program_id(0)

    @pl.when(step == 0)
    def _():
        out_ref[...] = jnp.zeros_like(out_ref)

    for i in range(PAIRS):
        pair = step * PAIRS + i
        target = pl.multiple_of(target_ref[pair] * BLOCK, BLOCK)
        columns = pl.ds(target, BLOCK)
        product = jnp.dot(
            source_ref[slot_ref[pair]], weight_ref[i], preferred_element_type=jnp.float32
        )
        out_ref[:, columns] += product

    @pl.when(step == pl.num_programs(0) - 1)
    def _():
        rows, cells = out_ref.shape
        total = jnp.zeros((rows, BLOCK), jnp.float32)
        for t in range(cells // BLOCK):
            columns = pl.ds(t * BLOCK, BLOCK)
            total += out_ref[:, columns] * area_ref[:, columns]
        mass_ref[...] = as_lanes(jnp.sum(total, axis=1, keepdims=True))


def regridded_blocks(pair_slot, pair_target, inbound, weights, area):
    slots, rows, _ = inbound.shape
    cells = area.shape[1]
    pairs = weights.shape[0]
    return pl.pallas_call(
        regrid,
        out_shape=(
            jax.ShapeDtypeStruct((rows, cells), jnp.float32),
            jax.ShapeDtypeStruct((1, rows), jnp.float32),
        ),
        grid_spec=pltpu.PrefetchScalarGridSpec(
            num_scalar_prefetch=2,
            grid=(pairs // PAIRS,),
            in_specs=[
                pl.BlockSpec((slots, rows, BLOCK), lambda i, s, t: (0, 0, 0)),
                pl.BlockSpec((PAIRS, BLOCK, BLOCK), lambda i, s, t: (i, 0, 0)),
                pl.BlockSpec((1, cells), lambda i, s, t: (0, 0)),
            ],
            out_specs=(
                pl.BlockSpec((rows, cells), lambda i, s, t: (0, 0)),
                pl.BlockSpec((1, rows), lambda i, s, t: (0, 0)),
            ),
        ),
    )(pair_slot, pair_target, inbound, weights, area)


def exchange(own_ref, sum_ref, all_ref, send_sem, recv_sem):
    here = [lax.axis_index(axis) for axis in AXES]
    sizes = SIZES
    me = ((here[0] * sizes[1] + here[1]) * sizes[2] + here[2]) * sizes[3] + here[3]
    peers = sizes[0] * sizes[1] * sizes[2] * sizes[3]

    def place(step):
        peer = lax.rem(me + step, peers)
        x = lax.rem(peer, sizes[3])
        y = lax.rem(peer // sizes[3], sizes[2])
        core = lax.rem(peer // (sizes[3] * sizes[2]), sizes[1])
        z = peer // (sizes[3] * sizes[2] * sizes[1])
        return (z, core, y, x)

    barrier = pltpu.get_barrier_semaphore()

    def greet(step, _):
        pl.semaphore_signal(
            barrier, inc=1, device_id=place(step), device_id_type=pl.DeviceIdType.MESH
        )
        return 0

    lax.fori_loop(1, peers, greet, 0)
    pl.semaphore_wait(barrier, peers - 1)

    def copy(step):
        return pltpu.make_async_remote_copy(
            src_ref=own_ref,
            dst_ref=all_ref.at[step],
            send_sem=send_sem.at[step],
            recv_sem=recv_sem.at[step],
            device_id=place(step),
            device_id_type=pl.DeviceIdType.MESH,
        )

    def send(step, _):
        copy(step).start()
        return 0

    lax.fori_loop(1, peers, send, 0)

    def arrive(step, _):
        copy(step).wait()
        return 0

    lax.fori_loop(1, peers, arrive, 0)
    total = own_ref[...]
    for step in range(1, peers):
        total += all_ref[step]
    sum_ref[...] = total


def summed(own):
    peers = SIZES[0] * SIZES[1] * SIZES[2] * SIZES[3]
    return pl.pallas_call(
        exchange,
        out_shape=jax.ShapeDtypeStruct(own.shape, own.dtype),
        in_specs=[pl.BlockSpec(memory_space=pltpu.VMEM)],
        out_specs=pl.BlockSpec(memory_space=pltpu.VMEM),
        scratch_shapes=[
            pltpu.VMEM((peers,) + own.shape, own.dtype),
            pltpu.SemaphoreType.DMA((peers,)),
            pltpu.SemaphoreType.DMA((peers,)),
        ],
        compiler_params=pltpu.CompilerParams(collective_id=1, has_side_effects=True),
    )(own)


def shards(src_field, src_area, tgt_area, weights, send_index, pair_slot, pair_target):
    rows = src_field.shape[0]
    peers, capacity = send_index.shape[1:]
    source_local = jnp.sum(src_field.astype(jnp.float32) * src_area[None, :], axis=1)
    outbound = outbound_blocks(send_index, src_field)
    outbound = outbound.reshape(peers, capacity, rows, BLOCK)
    inbound = lax.all_to_all(outbound, AXES, split_axis=0, concat_axis=0, tiled=True)
    inbound = inbound.reshape(peers * capacity, rows, BLOCK)
    regridded, target_local = regridded_blocks(
        pair_slot, pair_target, inbound, weights, tgt_area[None, :]
    )
    own = jnp.concatenate([source_local[None, :], target_local], axis=1)
    total = summed(own)
    scale = total[0, :rows] / total[0, rows:]
    return regridded * scale[:, None]


def solution(mesh):
    split = Mesh(mesh.devices.reshape(SIZES), AXES)
    placed = (
        P(None, AXES),
        P(AXES),
        P(AXES),
        P(AXES, None, None),
        P(AXES, None, None),
        P(AXES),
        P(AXES),
    )
    return jax.shard_map(
        shards, mesh=split, in_specs=placed, out_specs=P(None, AXES), check_vma=False
    )
```

```python
import itertools

import jax
import jax.numpy as jnp
from jax import lax
from jax.experimental import pallas as pl
from jax.experimental.pallas import tpu as pltpu
from jax.sharding import Mesh
from jax.sharding import PartitionSpec as P

AXES = ("z", "core", "y", "x")
SIZES = (4, 2, 4, 4)
BLOCK = 128
GATHERED = 32
PAIRS = 32


def collect(index_ref, source_ref, out_ref, held, in_sem, out_sem):
    slots = held.shape[0]
    groups = slots // GATHERED

    def span(group):
        return pl.ds(group * GATHERED, GATHERED)

    for slot in range(slots):
        block = jnp.maximum(index_ref[0, slot % 2, slot // 2], 0)
        columns = pl.ds(pl.multiple_of(block * BLOCK, BLOCK), BLOCK)
        pltpu.make_async_copy(
            source_ref.at[:, columns], held.at[slot], in_sem.at[slot // GATHERED]
        ).start()
    for group in range(groups):
        pltpu.make_async_copy(
            out_ref.at[span(group)], held.at[span(group)], in_sem.at[group]
        ).wait()
        pltpu.make_async_copy(
            held.at[span(group)], out_ref.at[span(group)], out_sem.at[group]
        ).start()
    for group in range(groups):
        pltpu.make_async_copy(
            held.at[span(group)], out_ref.at[span(group)], out_sem.at[group]
        ).wait()


def outbound_blocks(send_index, source):
    rows = source.shape[0]
    peers, capacity = send_index.shape[1:]
    slots = peers * capacity
    return pl.pallas_call(
        collect,
        out_shape=jax.ShapeDtypeStruct((slots, rows, BLOCK), source.dtype),
        in_specs=[
            pl.BlockSpec(memory_space=pltpu.SMEM),
            pl.BlockSpec(memory_space=pl.ANY),
        ],
        out_specs=pl.BlockSpec(memory_space=pl.ANY),
        scratch_shapes=[
            pltpu.VMEM((slots, rows, BLOCK), source.dtype),
            pltpu.SemaphoreType.DMA((slots // GATHERED,)),
            pltpu.SemaphoreType.DMA((slots // GATHERED,)),
        ],
    )(jnp.swapaxes(send_index, 1, 2), source)


def slot_weights(slot_ref, target_ref, area_ref, weight_ref, out_ref, sums, areas):
    step = pl.program_id(0)

    @pl.when(step == 0)
    def _():
        sums[...] = jnp.zeros_like(sums)
        area = area_ref[...]
        high = area.astype(jnp.bfloat16)
        low = (area - high.astype(jnp.float32)).astype(jnp.bfloat16)
        areas[:, 0:8, :] = jnp.broadcast_to(high[:, None, :], (area.shape[0], 8, BLOCK))
        areas[:, 8:16, :] = jnp.broadcast_to(low[:, None, :], (area.shape[0], 8, BLOCK))

    for i in range(PAIRS):
        pair = step * PAIRS + i
        product = lax.dot_general(
            areas[target_ref[pair]],
            weight_ref[i],
            (((1,), (1,)), ((), ())),
            preferred_element_type=jnp.float32,
        )
        sums[slot_ref[pair]] += product[0:8] + product[8:16]

    @pl.when(step == pl.num_programs(0) - 1)
    def _():
        out_ref[...] = sums[:, 0, :]


def weights_of_slots(pair_slot, pair_target, area, weights, slots):
    pairs = weights.shape[0]
    targets = area.shape[0]
    return pl.pallas_call(
        slot_weights,
        out_shape=jax.ShapeDtypeStruct((slots, BLOCK), jnp.float32),
        grid_spec=pltpu.PrefetchScalarGridSpec(
            num_scalar_prefetch=2,
            grid=(pairs // PAIRS,),
            in_specs=[
                pl.BlockSpec((targets, BLOCK), lambda i, s, t: (0, 0)),
                pl.BlockSpec((PAIRS, BLOCK, BLOCK), lambda i, s, t: (i, 0, 0)),
            ],
            out_specs=pl.BlockSpec((slots, BLOCK), lambda i, s, t: (0, 0)),
            scratch_shapes=[
                pltpu.VMEM((slots, 8, BLOCK), jnp.float32),
                pltpu.VMEM((targets, 16, BLOCK), jnp.bfloat16),
            ],
        ),
        cost_estimate=pl.CostEstimate(
            flops=2 * pairs * 64 * BLOCK * BLOCK,
            bytes_accessed=pairs * BLOCK * BLOCK * 2,
            transcendentals=0,
        ),
    )(pair_slot, pair_target, area, weights)


def as_lanes(column):
    rows = column.shape[0]
    wide = jnp.broadcast_to(column, (rows, BLOCK))
    return jnp.transpose(wide)[0:1, :]


def regrid(slot_ref, target_ref, source_ref, weight_ref, total_ref, out_ref):
    step = pl.program_id(0)

    @pl.when(step == 0)
    def _():
        out_ref[...] = jnp.zeros_like(out_ref)

    for i in range(PAIRS):
        pair = step * PAIRS + i
        target = pl.multiple_of(target_ref[pair] * BLOCK, BLOCK)
        columns = pl.ds(target, BLOCK)
        product = jnp.dot(
            source_ref[slot_ref[pair]], weight_ref[i], preferred_element_type=jnp.float32
        )
        out_ref[:, columns] += product

    @pl.when(step == pl.num_programs(0) - 1)
    def _():
        rows, cells = out_ref.shape
        total = jnp.transpose(jnp.broadcast_to(total_ref[...], (BLOCK, BLOCK)))
        scale = total[:rows] / total[rows : 2 * rows]
        for t in range(cells // BLOCK):
            columns = pl.ds(t * BLOCK, BLOCK)
            out_ref[:, columns] = out_ref[:, columns] * scale


def target_blocks(pair_slot, pair_target, inbound, weights, total, cells):
    slots, rows, _ = inbound.shape
    pairs = weights.shape[0]
    return pl.pallas_call(
        regrid,
        out_shape=jax.ShapeDtypeStruct((rows, cells), jnp.float32),
        grid_spec=pltpu.PrefetchScalarGridSpec(
            num_scalar_prefetch=2,
            grid=(pairs // PAIRS,),
            in_specs=[
                pl.BlockSpec((slots, rows, BLOCK), lambda i, s, t: (0, 0, 0)),
                pl.BlockSpec((PAIRS, BLOCK, BLOCK), lambda i, s, t: (i, 0, 0)),
                pl.BlockSpec((1, BLOCK), lambda i, s, t: (0, 0)),
            ],
            out_specs=pl.BlockSpec((rows, cells), lambda i, s, t: (0, 0)),
        ),
    )(pair_slot, pair_target, inbound, weights, total)


def masses(
    slot_ref, source_ref, block_ref, total_ref,
    back, own, others, send_sem, back_sem, mass_send_sem, mass_sem,
):
    here = [lax.axis_index(axis) for axis in AXES]
    turned = [[lax.rem(h + k, size) for k in range(size)] for h, size in zip(here, SIZES)]
    peers = SIZES[0] * SIZES[1] * SIZES[2] * SIZES[3]

    def number(place):
        value = place[0]
        for size, part in zip(SIZES[1:], place[1:]):
            value = value * size + part
        return value

    places = [
        tuple(axis[k] for axis, k in zip(turned, offset))
        for offset in itertools.product(*(range(size) for size in SIZES))
    ][1:]
    me = number(here)
    barrier = pltpu.get_barrier_semaphore()
    for place in places:
        pl.semaphore_signal(
            barrier, inc=1, device_id=place, device_id_type=pl.DeviceIdType.MESH
        )
    pl.semaphore_wait(barrier, peers - 1)
    for place in places:
        pltpu.make_async_remote_copy(
            src_ref=slot_ref.at[number(place)],
            dst_ref=back.at[me],
            send_sem=send_sem,
            recv_sem=back_sem,
            device_id=place,
            device_id_type=pl.DeviceIdType.MESH,
        ).start()
    back[me] = slot_ref[me]
    most = pl.ds(0, peers - 1)
    pltpu.make_async_copy(slot_ref.at[most], back.at[most], back_sem).wait()
    pltpu.make_async_copy(slot_ref.at[most], back.at[most], send_sem).wait()
    rows = block_ref.shape[2]

    def add(peer, total):
        for slot in range(block_ref.shape[1]):
            factors = back[peer, pl.ds(slot, 1), :]
            total += block_ref[peer, slot].astype(jnp.float32) * factors
        return total

    total = lax.fori_loop(0, peers, add, jnp.zeros((rows, BLOCK), jnp.float32), unroll=4)
    target = as_lanes(jnp.sum(total, axis=1, keepdims=True))
    own[...] = jnp.concatenate([source_ref[...], target], axis=1)
    others[me] = own[...]
    for place in places:
        pltpu.make_async_remote_copy(
            src_ref=own,
            dst_ref=others.at[me],
            send_sem=mass_send_sem,
            recv_sem=mass_sem,
            device_id=place,
            device_id_type=pl.DeviceIdType.MESH,
        ).start()
    pltpu.make_async_copy(others.at[most], others.at[most], mass_sem).wait()
    pltpu.make_async_copy(others.at[most], others.at[most], mass_send_sem).wait()
    total = others[0]
    for peer in range(1, peers):
        total += others[peer]
    total_ref[...] = total


def total_masses(slot_sums, source_local, outbound):
    peers, capacity, rows, _ = outbound.shape
    return pl.pallas_call(
        masses,
        out_shape=jax.ShapeDtypeStruct((1, 2 * rows), jnp.float32),
        in_specs=[pl.BlockSpec(memory_space=pltpu.VMEM)] * 3,
        out_specs=pl.BlockSpec(memory_space=pltpu.VMEM),
        scratch_shapes=[
            pltpu.VMEM((peers, capacity, BLOCK), jnp.float32),
            pltpu.VMEM((1, 2 * rows), jnp.float32),
            pltpu.VMEM((peers, 1, 2 * rows), jnp.float32),
        ]
        + [pltpu.SemaphoreType.DMA] * 4,
        compiler_params=pltpu.CompilerParams(collective_id=1, has_side_effects=True),
        cost_estimate=pl.CostEstimate(
            flops=2 * 400 * 64 * BLOCK * BLOCK, bytes_accessed=4194304, transcendentals=0
        ),
    )(slot_sums, source_local, outbound)


def shards(src_field, src_area, tgt_area, weights, send_index, pair_slot, pair_target):
    rows = src_field.shape[0]
    peers, capacity = send_index.shape[1:]
    source_local = jnp.sum(src_field.astype(jnp.float32) * src_area[None, :], axis=1)
    outbound = outbound_blocks(send_index, src_field)
    outbound = outbound.reshape(peers, capacity, rows, BLOCK)
    slot_sums = weights_of_slots(
        pair_slot, pair_target, tgt_area.reshape(-1, BLOCK), weights, peers * capacity
    )
    slot_sums = slot_sums.reshape(peers, capacity, BLOCK)
    total = total_masses(slot_sums, source_local[None, :], outbound)
    inbound = lax.all_to_all(outbound, AXES, split_axis=0, concat_axis=0, tiled=True)
    inbound = inbound.reshape(peers * capacity, rows, BLOCK)
    return target_blocks(
        pair_slot, pair_target, inbound, weights, total, tgt_area.shape[0]
    )


def solution(mesh):
    split = Mesh(mesh.devices.reshape(SIZES), AXES)
    placed = (
        P(None, AXES),
        P(AXES),
        P(AXES),
        P(AXES, None, None),
        P(AXES, None, None),
        P(AXES),
        P(AXES),
    )
    return jax.shard_map(
        shards, mesh=split, in_specs=placed, out_specs=P(None, AXES), check_vma=False
    )
```

```python
import itertools

import jax
import jax.numpy as jnp
from jax import lax
from jax.experimental import pallas as pl
from jax.experimental.pallas import tpu as pltpu
from jax.sharding import Mesh
from jax.sharding import PartitionSpec as P

AXES = ("z", "core", "y", "x")
SIZES = (4, 2, 4, 4)
PEERS = 128
BLOCK = 128
GATHERED = 32
PAIRS = 32
EARLY = 40
MESH = pl.DeviceIdType.MESH
ANY = pl.BlockSpec(memory_space=pl.ANY)
SMEM = pl.BlockSpec(memory_space=pltpu.SMEM)
VMEM = pl.BlockSpec(memory_space=pltpu.VMEM)


def chunk(index, size):
    return pl.ds(pl.multiple_of(index * size, size), size)


def prepare(
    index_ref, slot_ref, target_ref, area_ref, source_ref, weight_ref, out_ref, sum_ref,
    held, weights, sums, areas, in_sem, out_sem, weight_sem,
):
    slots = held.shape[0]
    pairs = weights.shape[0]

    for slot in range(slots):
        block = jnp.maximum(index_ref[0, slot % 2, slot // 2], 0)
        columns = pl.ds(pl.multiple_of(block * BLOCK, BLOCK), BLOCK)
        pltpu.make_async_copy(
            source_ref.at[:, columns], held.at[slot], in_sem.at[slot // GATHERED]
        ).start()
    for part in range(pairs // PAIRS):
        span = pl.ds(part * PAIRS, PAIRS)
        pltpu.make_async_copy(
            weight_ref.at[span], weights.at[span], weight_sem.at[part]
        ).start()
    sums[...] = jnp.zeros_like(sums)
    area = area_ref[...]
    high = area.astype(jnp.bfloat16)
    low = (area - high.astype(jnp.float32)).astype(jnp.bfloat16)
    areas[:, 0:8, :] = jnp.broadcast_to(high[:, None, :], (area.shape[0], 8, BLOCK))
    areas[:, 8:16, :] = jnp.broadcast_to(low[:, None, :], (area.shape[0], 8, BLOCK))
    for group in range(slots // GATHERED):
        span = pl.ds(group * GATHERED, GATHERED)
        pltpu.make_async_copy(out_ref.at[span], held.at[span], in_sem.at[group]).wait()
        pltpu.make_async_copy(held.at[span], out_ref.at[span], out_sem.at[group]).start()

    def part_of(part, _):
        span = chunk(part, PAIRS)
        pltpu.make_async_copy(
            weight_ref.at[span], weights.at[span], weight_sem.at[part]
        ).wait()
        for i in range(PAIRS):
            pair = part * PAIRS + i
            product = lax.dot_general(
                areas[target_ref[pair]],
                weights[pair],
                (((1,), (1,)), ((), ())),
                preferred_element_type=jnp.float32,
            )
            sums[slot_ref[pair]] += product[0:8] + product[8:16]
        return 0

    lax.fori_loop(0, pairs // PAIRS, part_of, 0)
    sum_ref[...] = sums[:, 0, :]
    for group in range(slots // GATHERED):
        span = pl.ds(group * GATHERED, GATHERED)
        pltpu.make_async_copy(held.at[span], out_ref.at[span], out_sem.at[group]).wait()


def prepared(send_index, pair_slot, pair_target, area, source, weights):
    rows = source.shape[0]
    peers, capacity = send_index.shape[1:]
    slots = peers * capacity
    targets = area.shape[0]
    pairs = weights.shape[0]
    return pl.pallas_call(
        prepare,
        out_shape=(
            jax.ShapeDtypeStruct((slots, rows, BLOCK), source.dtype),
            jax.ShapeDtypeStruct((slots, BLOCK), jnp.float32),
        ),
        in_specs=[SMEM, SMEM, SMEM, VMEM, ANY, ANY],
        out_specs=(ANY, VMEM),
        scratch_shapes=[
            pltpu.VMEM((slots, rows, BLOCK), source.dtype),
            pltpu.VMEM(weights.shape, weights.dtype),
            pltpu.VMEM((slots, 8, BLOCK), jnp.float32),
            pltpu.VMEM((targets, 16, BLOCK), jnp.bfloat16),
            pltpu.SemaphoreType.DMA((slots // GATHERED,)),
            pltpu.SemaphoreType.DMA((slots // GATHERED,)),
            pltpu.SemaphoreType.DMA((pairs // PAIRS,)),
        ],
    )(jnp.swapaxes(send_index, 1, 2), pair_slot, pair_target, area, source, weights)


def as_lanes(column):
    rows = column.shape[0]
    wide = jnp.broadcast_to(column, (rows, BLOCK))
    return jnp.transpose(wide)[0:1, :]


def routes():
    left = [offset for offset in itertools.product(*(range(size) for size in SIZES))][1:]

    def load(offset):
        links = [0] * 6
        for axis, step in enumerate((offset[0], offset[2], offset[3])):
            links[2 * axis] += step in (1, 2)
            links[2 * axis + 1] += step in (2, 3)
        return links

    used = [0] * 6
    order = []
    while left:
        def spread(offset):
            after = [a + b for a, b in zip(used, load(offset))]
            return max(after) - min(after)

        best = min(left, key=spread)
        left.remove(best)
        used = [a + b for a, b in zip(used, load(best))]
        order.append(best)
    return order


def exchange(
    slot_ref, source_ref, area_ref, block_ref, in_ref, total_ref,
    back, own, others, blocks, source,
    send_sem, recv_sem, near_sem, block_sem, source_sem,
    back_send_sem, back_sem, mass_send_sem, mass_sem,
):
    here = [lax.axis_index(axis) for axis in AXES]
    turned = [[lax.rem(h + k, size) for k in range(size)] for h, size in zip(here, SIZES)]

    def number(place):
        value = place[0]
        for size, part in zip(SIZES[1:], place[1:]):
            value = value * size + part
        return value

    places = [
        tuple(axis[k] for axis, k in zip(turned, offset)) for offset in routes()
    ]
    me = number(here)
    capacity, rows = block_ref.shape[1:3]
    barrier = pltpu.get_barrier_semaphore()
    for place in places:
        pl.semaphore_signal(barrier, inc=1, device_id=place, device_id_type=MESH)
    near = pltpu.make_async_copy(block_ref, blocks, block_sem)
    near.start()
    far = pltpu.make_async_copy(source_ref, source, source_sem)
    far.start()
    back[me] = slot_ref[me]
    pl.semaphore_wait(barrier, PEERS - 1)

    for place in places:
        pltpu.make_async_remote_copy(
            src_ref=slot_ref.at[number(place)],
            dst_ref=back.at[me],
            send_sem=back_send_sem,
            recv_sem=back_sem,
            device_id=place,
            device_id_type=MESH,
        ).start()

    def send(place):
        pltpu.make_async_remote_copy(
            src_ref=block_ref.at[number(place)],
            dst_ref=in_ref.at[me],
            send_sem=send_sem,
            recv_sem=recv_sem,
            device_id=place,
            device_id_type=MESH,
        ).start()

    for place in places[:EARLY]:
        send(place)

    near.wait()
    kept = pltpu.make_async_copy(blocks.at[me], in_ref.at[me], near_sem)
    kept.start()
    far.wait()

    def source_part(part, total):
        columns = chunk(part, BLOCK)
        return total + source[:, columns].astype(jnp.float32) * area_ref[:, columns]

    zero = jnp.zeros((rows, BLOCK), jnp.float32)
    count = source.shape[1] // BLOCK
    source_total = lax.fori_loop(0, count, source_part, zero, unroll=8)
    most = pl.ds(0, PEERS - 1)
    pltpu.make_async_copy(slot_ref.at[most], back.at[most], back_sem).wait()

    def target_part(peer, total):
        for slot in range(capacity):
            factors = back[peer, pl.ds(slot, 1), :]
            total += blocks[peer, slot].astype(jnp.float32) * factors
        return total

    target_total = lax.fori_loop(0, PEERS, target_part, zero, unroll=4)
    column = jnp.concatenate(
        [
            jnp.sum(source_total, axis=1, keepdims=True),
            jnp.sum(target_total, axis=1, keepdims=True),
        ],
        axis=0,
    )
    own[...] = as_lanes(column)
    others[me] = own[...]
    for place in places:
        pltpu.make_async_remote_copy(
            src_ref=own,
            dst_ref=others.at[me],
            send_sem=mass_send_sem,
            recv_sem=mass_sem,
            device_id=place,
            device_id_type=MESH,
        ).start()
    for place in places[EARLY:]:
        send(place)
    pltpu.make_async_copy(others.at[most], others.at[most], mass_sem).wait()
    total = others[0]
    for peer in range(1, PEERS):
        total += others[peer]
    total_ref[...] = total
    pltpu.make_async_copy(others.at[most], others.at[most], mass_send_sem).wait()
    pltpu.make_async_copy(slot_ref.at[most], back.at[most], back_send_sem).wait()
    kept.wait()
    pltpu.make_async_copy(block_ref.at[most], in_ref.at[most], send_sem).wait()
    pltpu.make_async_copy(block_ref.at[most], in_ref.at[most], recv_sem).wait()


def exchanged(slot_sums, source, area, outbound):
    peers, capacity, rows, _ = outbound.shape
    return pl.pallas_call(
        exchange,
        out_shape=(
            jax.ShapeDtypeStruct(outbound.shape, outbound.dtype),
            jax.ShapeDtypeStruct((1, 2 * rows), jnp.float32),
        ),
        in_specs=[VMEM, ANY, VMEM, ANY],
        out_specs=(ANY, VMEM),
        scratch_shapes=[
            pltpu.VMEM((peers, capacity, BLOCK), jnp.float32),
            pltpu.VMEM((1, 2 * rows), jnp.float32),
            pltpu.VMEM((peers, 1, 2 * rows), jnp.float32),
            pltpu.VMEM(outbound.shape, outbound.dtype),
            pltpu.VMEM(source.shape, source.dtype),
        ]
        + [pltpu.SemaphoreType.DMA] * 9,
        compiler_params=pltpu.CompilerParams(collective_id=1, has_side_effects=True),
    )(slot_sums, source, area, outbound)


def regrid(
    slot_ref, target_ref, total_ref, source_ref, weight_ref, out_ref,
    source, weights, source_sem, weight_sem,
):
    pairs = weights.shape[0]
    far = pltpu.make_async_copy(source_ref, source, source_sem)
    far.start()
    for part in range(pairs // PAIRS):
        span = pl.ds(part * PAIRS, PAIRS)
        pltpu.make_async_copy(
            weight_ref.at[span], weights.at[span], weight_sem.at[part]
        ).start()
    out_ref[...] = jnp.zeros_like(out_ref)
    far.wait()

    def part_of(part, _):
        span = chunk(part, PAIRS)
        pltpu.make_async_copy(
            weight_ref.at[span], weights.at[span], weight_sem.at[part]
        ).wait()
        for i in range(PAIRS):
            pair = part * PAIRS + i
            product = jnp.dot(
                source[slot_ref[pair]], weights[pair], preferred_element_type=jnp.float32
            )
            out_ref[:, chunk(target_ref[pair], BLOCK)] += product
        return 0

    lax.fori_loop(0, pairs // PAIRS, part_of, 0)
    rows, cells = out_ref.shape
    total = jnp.transpose(jnp.broadcast_to(total_ref[...], (BLOCK, BLOCK)))
    scale = total[:rows] / total[rows : 2 * rows]
    for t in range(cells // BLOCK):
        columns = pl.ds(t * BLOCK, BLOCK)
        out_ref[:, columns] = out_ref[:, columns] * scale


def target_blocks(pair_slot, pair_target, inbound, weights, total, cells):
    slots, rows, _ = inbound.shape
    pairs = weights.shape[0]
    return pl.pallas_call(
        regrid,
        out_shape=jax.ShapeDtypeStruct((rows, cells), jnp.float32),
        in_specs=[SMEM, SMEM, VMEM, ANY, ANY],
        out_specs=VMEM,
        scratch_shapes=[
            pltpu.VMEM(inbound.shape, inbound.dtype),
            pltpu.VMEM(weights.shape, weights.dtype),
            pltpu.SemaphoreType.DMA,
            pltpu.SemaphoreType.DMA((pairs // PAIRS,)),
        ],
    )(pair_slot, pair_target, total, inbound, weights)


def shards(src_field, src_area, tgt_area, weights, send_index, pair_slot, pair_target):
    rows = src_field.shape[0]
    peers, capacity = send_index.shape[1:]
    outbound, slot_sums = prepared(
        send_index, pair_slot, pair_target, tgt_area.reshape(-1, BLOCK), src_field, weights
    )
    inbound, total = exchanged(
        slot_sums.reshape(peers, capacity, BLOCK),
        src_field,
        src_area[None, :],
        outbound.reshape(peers, capacity, rows, BLOCK),
    )
    inbound = inbound.reshape(peers * capacity, rows, BLOCK)
    return target_blocks(
        pair_slot, pair_target, inbound, weights, total, tgt_area.shape[0]
    )


def solution(mesh):
    split = Mesh(mesh.devices.reshape(SIZES), AXES)
    placed = (
        P(None, AXES),
        P(AXES),
        P(AXES),
        P(AXES, None, None),
        P(AXES, None, None),
        P(AXES),
        P(AXES),
    )
    return jax.shard_map(
        shards, mesh=split, in_specs=placed, out_specs=P(None, AXES), check_vma=False
    )
```

```python
import itertools

import jax
import jax.numpy as jnp
from jax import lax
from jax.experimental import pallas as pl
from jax.experimental.pallas import tpu as pltpu
from jax.sharding import Mesh
from jax.sharding import PartitionSpec as P

AXES = ("z", "core", "y", "x")
SIZES = (4, 2, 4, 4)
PEERS = 128
BLOCK = 128
PAIRS = 32
EARLY = 32
MIDDLE = 64
AHEAD = 4
MESH = pl.DeviceIdType.MESH
ANY = pl.BlockSpec(memory_space=pl.ANY)
SMEM = pl.BlockSpec(memory_space=pltpu.SMEM)
VMEM = pl.BlockSpec(memory_space=pltpu.VMEM)


def chunk(index, size):
    return pl.ds(pl.multiple_of(index * size, size), size)


def as_lanes(column):
    rows = column.shape[0]
    wide = jnp.broadcast_to(column, (rows, BLOCK))
    return jnp.transpose(wide)[0:1, :]


def routes():
    left = [offset for offset in itertools.product(*(range(size) for size in SIZES))][1:]

    def load(offset):
        links = [0] * 6
        for axis, step in enumerate((offset[0], offset[2], offset[3])):
            links[2 * axis] += step in (1, 2)
            links[2 * axis + 1] += step in (2, 3)
        return links

    used = [0] * 6
    order = []
    while left:
        def spread(offset):
            after = [a + b for a, b in zip(used, load(offset))]
            return max(after) - min(after)

        best = min(left, key=spread)
        left.remove(best)
        used = [a + b for a, b in zip(used, load(best))]
        order.append(best)
    return order


def three_terms(value):
    terms = []
    for _ in range(3):
        term = value.astype(jnp.bfloat16)
        terms.append(term)
        value = value - term.astype(jnp.float32)
    return terms


def exchange(
    index_ref, target_ref, slot_ref, target_area_ref, area_ref, source_ref, weight_ref,
    in_ref, total_ref,
    source, weights, blocks, areas, pair_rows, slot_rows, back, own, others,
    send_sem, recv_sem, near_sem, source_sem, weight_sem,
    back_send_sem, back_sem, mass_send_sem, mass_sem,
):
    here = [lax.axis_index(axis) for axis in AXES]
    turned = [[lax.rem(h + k, size) for k in range(size)] for h, size in zip(here, SIZES)]
    offsets = routes()
    opposite = [
        offsets.index(tuple((-k) % size for k, size in zip(offset, SIZES)))
        for offset in offsets
    ]

    def number(place):
        value = place[0]
        for size, part in zip(SIZES[1:], place[1:]):
            value = value * size + part
        return value

    places = [tuple(axis[k] for axis, k in zip(turned, offset)) for offset in offsets]
    me = number(here)
    last = PEERS - 1
    rows = source.shape[0]
    pairs = weights.shape[0]
    barrier = pltpu.get_barrier_semaphore()
    far = pltpu.make_async_copy(source_ref, source, source_sem)
    far.start()
    for place in places:
        pl.semaphore_signal(barrier, inc=1, device_id=place, device_id_type=MESH)
    for part in range(pairs // PAIRS):
        span = pl.ds(part * PAIRS, PAIRS)
        pltpu.make_async_copy(
            weight_ref.at[span], weights.at[span], weight_sem.at[part]
        ).start()

    def gather(k):
        peer = me if k == last else number(places[k])
        for slot in range(blocks.shape[1]):
            block = jnp.maximum(index_ref[0, slot, peer], 0)
            blocks[k, slot] = source[:, pl.ds(block * BLOCK, BLOCK)]

    def send(k):
        pltpu.make_async_remote_copy(
            src_ref=blocks.at[k],
            dst_ref=in_ref.at[me],
            send_sem=send_sem,
            recv_sem=recv_sem,
            device_id=places[k],
            device_id_type=MESH,
        ).start()

    far.wait()
    for k in range(EARLY):
        gather(k)
    pl.semaphore_wait(barrier, PEERS - 1)
    for k in range(EARLY):
        send(k)
    for k in range(EARLY, PEERS):
        gather(k)
    kept = pltpu.make_async_copy(blocks.at[last], in_ref.at[me], near_sem)
    kept.start()

    area = target_area_ref[...]
    high = area.astype(jnp.bfloat16)
    low = (area - high.astype(jnp.float32)).astype(jnp.bfloat16)
    areas[:, 0:8, :] = jnp.broadcast_to(high[:, None, :], (area.shape[0], 8, BLOCK))
    areas[:, 8:16, :] = jnp.broadcast_to(low[:, None, :], (area.shape[0], 8, BLOCK))

    def part_of(part, _):
        span = chunk(part, PAIRS)
        pltpu.make_async_copy(
            weight_ref.at[span], weights.at[span], weight_sem.at[part]
        ).wait()
        for i in range(PAIRS):
            pair = part * PAIRS + i
            product = lax.dot_general(
                areas[target_ref[pair]],
                weights[pair],
                (((1,), (1,)), ((), ())),
                preferred_element_type=jnp.float32,
            )
            row = product[0:8] + product[8:16]
            pair_rows[pl.ds(pair, 1), :] = row[0:1]
        return 0

    lax.fori_loop(0, pairs // PAIRS, part_of, 0)
    terms = three_terms(pair_rows[...])
    peer = lax.broadcasted_iota(jnp.int32, (PEERS, pairs), 0)
    capacity = blocks.shape[1]
    for slot in range(capacity):
        chosen = jnp.where(peer * capacity + slot == slot_ref[...], 1.0, 0.0)
        chosen = chosen.astype(jnp.bfloat16)
        slot_rows[:, slot, :] = sum(
            jnp.dot(chosen, term, preferred_element_type=jnp.float32) for term in terms
        )
    back[last] = slot_rows[me]
    for k in range(last):
        pltpu.make_async_remote_copy(
            src_ref=slot_rows.at[number(places[k])],
            dst_ref=back.at[opposite[k]],
            send_sem=back_send_sem,
            recv_sem=back_sem,
            device_id=places[k],
            device_id_type=MESH,
        ).start()
    for k in range(EARLY, MIDDLE):
        send(k)

    def source_part(part, total):
        columns = chunk(part, BLOCK)
        return total + source[:, columns].astype(jnp.float32) * area_ref[:, columns]

    zero = jnp.zeros((rows, BLOCK), jnp.float32)
    count = source.shape[1] // BLOCK
    source_total = lax.fori_loop(0, count, source_part, zero, unroll=8)
    most = pl.ds(0, last)
    pltpu.make_async_copy(slot_rows.at[most], back.at[most], back_sem).wait()

    def target_part(peer, total):
        for slot in range(capacity):
            factors = back[peer, pl.ds(slot, 1), :]
            total += blocks[peer, slot].astype(jnp.float32) * factors
        return total

    target_total = lax.fori_loop(0, PEERS, target_part, zero, unroll=4)
    column = jnp.concatenate(
        [
            jnp.sum(source_total, axis=1, keepdims=True),
            jnp.sum(target_total, axis=1, keepdims=True),
        ],
        axis=0,
    )
    own[...] = as_lanes(column)
    others[me] = own[...]
    for k in range(last):
        pltpu.make_async_remote_copy(
            src_ref=own,
            dst_ref=others.at[me],
            send_sem=mass_send_sem,
            recv_sem=mass_sem,
            device_id=places[k],
            device_id_type=MESH,
        ).start()
    for k in range(MIDDLE, last):
        send(k)
    pltpu.make_async_copy(others.at[most], others.at[most], mass_sem).wait()
    total = others[0]
    for k in range(1, PEERS):
        total += others[k]
    total_ref[...] = total
    pltpu.make_async_copy(others.at[most], others.at[most], mass_send_sem).wait()
    pltpu.make_async_copy(slot_rows.at[most], back.at[most], back_send_sem).wait()
    kept.wait()
    pltpu.make_async_copy(blocks.at[most], in_ref.at[most], send_sem).wait()
    pltpu.make_async_copy(blocks.at[most], in_ref.at[most], recv_sem).wait()


def exchanged(send_index, pair_slot, pair_target, target_area, area, source, weights):
    rows = source.shape[0]
    peers, capacity = send_index.shape[1:]
    targets = target_area.shape[0]
    pairs = weights.shape[0]
    blocks = (peers, capacity, rows, BLOCK)
    return pl.pallas_call(
        exchange,
        out_shape=(
            jax.ShapeDtypeStruct(blocks, source.dtype),
            jax.ShapeDtypeStruct((1, 2 * rows), jnp.float32),
        ),
        in_specs=[SMEM, SMEM, VMEM, VMEM, VMEM, ANY, ANY],
        out_specs=(ANY, VMEM),
        scratch_shapes=[
            pltpu.VMEM(source.shape, source.dtype),
            pltpu.VMEM(weights.shape, weights.dtype),
            pltpu.VMEM(blocks, source.dtype),
            pltpu.VMEM((targets, 16, BLOCK), jnp.bfloat16),
            pltpu.VMEM((pairs, BLOCK), jnp.float32),
            pltpu.VMEM((peers, capacity, BLOCK), jnp.float32),
            pltpu.VMEM((peers, capacity, BLOCK), jnp.float32),
            pltpu.VMEM((1, 2 * rows), jnp.float32),
            pltpu.VMEM((peers, 1, 2 * rows), jnp.float32),
        ]
        + [pltpu.SemaphoreType.DMA] * 4
        + [pltpu.SemaphoreType.DMA((pairs // PAIRS,))]
        + [pltpu.SemaphoreType.DMA] * 4,
        compiler_params=pltpu.CompilerParams(collective_id=1, has_side_effects=True),
    )(
        jnp.swapaxes(send_index, 1, 2),
        pair_target,
        pair_slot[None, :],
        target_area,
        area,
        source,
        weights,
    )


def regrid(
    slot_ref, target_ref, total_ref, source_ref, weight_ref, out_ref,
    source, weights, source_sem, weight_sem,
):
    parts = weights.shape[0] // PAIRS

    def fetch(part):
        span = chunk(part, PAIRS)
        return pltpu.make_async_copy(
            weight_ref.at[span], weights.at[span], weight_sem.at[part]
        )

    far = pltpu.make_async_copy(source_ref, source, source_sem)
    far.start()
    for part in range(AHEAD):
        fetch(part).start()
    out_ref[...] = jnp.zeros_like(out_ref)
    far.wait()

    def part_of(part, _):
        @pl.when(part + AHEAD < parts)
        def _():
            fetch(part + AHEAD).start()

        fetch(part).wait()
        for i in range(PAIRS):
            pair = part * PAIRS + i
            product = jnp.dot(
                source[slot_ref[pair]], weights[pair], preferred_element_type=jnp.float32
            )
            out_ref[:, chunk(target_ref[pair], BLOCK)] += product
        return 0

    lax.fori_loop(0, parts, part_of, 0)
    rows, cells = out_ref.shape
    total = jnp.transpose(jnp.broadcast_to(total_ref[...], (BLOCK, BLOCK)))
    scale = total[:rows] / total[rows : 2 * rows]
    for t in range(cells // BLOCK):
        columns = pl.ds(t * BLOCK, BLOCK)
        out_ref[:, columns] = out_ref[:, columns] * scale


def target_blocks(pair_slot, pair_target, inbound, weights, total, cells):
    slots, rows, _ = inbound.shape
    pairs = weights.shape[0]
    return pl.pallas_call(
        regrid,
        out_shape=jax.ShapeDtypeStruct((rows, cells), jnp.float32),
        in_specs=[SMEM, SMEM, VMEM, ANY, ANY],
        out_specs=VMEM,
        scratch_shapes=[
            pltpu.VMEM(inbound.shape, inbound.dtype),
            pltpu.VMEM(weights.shape, weights.dtype),
            pltpu.SemaphoreType.DMA,
            pltpu.SemaphoreType.DMA((pairs // PAIRS,)),
        ],
    )(pair_slot, pair_target, total, inbound, weights)


def shards(src_field, src_area, tgt_area, weights, send_index, pair_slot, pair_target):
    rows = src_field.shape[0]
    peers, capacity = send_index.shape[1:]
    inbound, total = exchanged(
        send_index,
        pair_slot,
        pair_target,
        tgt_area.reshape(-1, BLOCK),
        src_area[None, :],
        src_field,
        weights,
    )
    inbound = inbound.reshape(peers * capacity, rows, BLOCK)
    return target_blocks(
        pair_slot, pair_target, inbound, weights, total, tgt_area.shape[0]
    )


def solution(mesh):
    split = Mesh(mesh.devices.reshape(SIZES), AXES)
    placed = (
        P(None, AXES),
        P(AXES),
        P(AXES),
        P(AXES, None, None),
        P(AXES, None, None),
        P(AXES),
        P(AXES),
    )
    return jax.shard_map(
        shards, mesh=split, in_specs=placed, out_specs=P(None, AXES), check_vma=False
    )
```

```python
import itertools

import jax
import jax.numpy as jnp
from jax import lax
from jax.experimental import pallas as pl
from jax.experimental.pallas import tpu as pltpu
from jax.sharding import Mesh
from jax.sharding import PartitionSpec as P

AXES = ("z", "core", "y", "x")
SIZES = (4, 2, 4, 4)
PEERS = 128
BLOCK = 128
PAIRS = 32
EARLY = 32
MIDDLE = 64
EXCHANGE_VMEM = 36 * 1024 * 1024
REGRID_VMEM = 24 * 1024 * 1024
MESH = pl.DeviceIdType.MESH
ANY = pl.BlockSpec(memory_space=pl.ANY)
HBM = pl.BlockSpec(memory_space=pltpu.HBM)
SMEM = pl.BlockSpec(memory_space=pltpu.SMEM)
VMEM = pl.BlockSpec(memory_space=pltpu.VMEM)


def chunk(index, size):
    return pl.ds(pl.multiple_of(index * size, size), size)


def as_lanes(column):
    rows = column.shape[0]
    wide = jnp.broadcast_to(column, (rows, BLOCK))
    return jnp.transpose(wide)[0:1, :]


def routes():
    left = [offset for offset in itertools.product(*(range(size) for size in SIZES))][1:]

    def load(offset):
        links = [0] * 6
        for axis, step in enumerate((offset[0], offset[2], offset[3])):
            links[2 * axis] += step in (1, 2)
            links[2 * axis + 1] += step in (2, 3)
        return links

    used = [0] * 6
    order = []
    while left:
        def spread(offset):
            after = [a + b for a, b in zip(used, load(offset))]
            return max(after) - min(after)

        best = min(left, key=spread)
        left.remove(best)
        used = [a + b for a, b in zip(used, load(best))]
        order.append(best)
    return order


def three_terms(value):
    terms = []
    for _ in range(3):
        term = value.astype(jnp.bfloat16)
        terms.append(term)
        value = value - term.astype(jnp.float32)
    return terms


def exchange(
    index_hbm, target_hbm, slot_hbm, target_area_hbm, area_hbm, source_ref, weight_ref,
    in_ref, total_ref, weights,
    index_ref, target_ref, slot_ref, target_area_ref, area_ref,
    source, blocks, areas, pair_rows, slot_rows, back, own, others,
    send_sem, recv_sem, source_sem, weight_sem, small_sem,
    back_send_sem, back_sem, mass_send_sem, mass_sem,
):
    here = [lax.axis_index(axis) for axis in AXES]
    turned = [[lax.rem(h + k, size) for k in range(size)] for h, size in zip(here, SIZES)]
    offsets = routes()
    opposite = [
        offsets.index(tuple((-k) % size for k, size in zip(offset, SIZES)))
        for offset in offsets
    ]

    def number(place):
        value = place[0]
        for size, part in zip(SIZES[1:], place[1:]):
            value = value * size + part
        return value

    places = [tuple(axis[k] for axis, k in zip(turned, offset)) for offset in offsets]
    me = number(here)
    last = PEERS - 1
    rows = source.shape[0]
    pairs = weights.shape[0]
    barrier = pltpu.get_barrier_semaphore()
    far = pltpu.make_async_copy(source_ref, source, source_sem)
    far.start()
    small = [
        pltpu.make_async_copy(whole, held, small_sem.at[i])
        for i, (whole, held) in enumerate(
            (
                (index_hbm, index_ref),
                (target_hbm, target_ref),
                (slot_hbm, slot_ref),
                (target_area_hbm, target_area_ref),
                (area_hbm, area_ref),
            )
        )
    ]
    for copy in small:
        copy.start()
    for place in places:
        pl.semaphore_signal(barrier, inc=1, device_id=place, device_id_type=MESH)
    def gather(k):
        peer = me if k == last else number(places[k])
        for slot in range(blocks.shape[1]):
            block = jnp.maximum(index_ref[0, slot, peer], 0)
            blocks[k, slot] = source[:, pl.ds(block * BLOCK, BLOCK)]

    def send(k):
        pltpu.make_async_remote_copy(
            src_ref=blocks.at[k],
            dst_ref=in_ref.at[me],
            send_sem=send_sem,
            recv_sem=recv_sem,
            device_id=places[k],
            device_id_type=MESH,
        ).start()

    for copy in small:
        copy.wait()
    far.wait()
    for part in range(pairs // PAIRS):
        span = pl.ds(part * PAIRS, PAIRS)
        pltpu.make_async_copy(
            weight_ref.at[span], weights.at[span], weight_sem.at[part]
        ).start()
    for k in range(EARLY):
        gather(k)
    pl.semaphore_wait(barrier, PEERS - 1)
    for k in range(EARLY):
        send(k)
    for k in range(EARLY, PEERS):
        gather(k)
    in_ref[me] = blocks[last]

    area = target_area_ref[...]
    high = area.astype(jnp.bfloat16)
    low = (area - high.astype(jnp.float32)).astype(jnp.bfloat16)
    areas[:, 0:8, :] = jnp.broadcast_to(high[:, None, :], (area.shape[0], 8, BLOCK))
    areas[:, 8:16, :] = jnp.broadcast_to(low[:, None, :], (area.shape[0], 8, BLOCK))

    def part_of(part, _):
        span = chunk(part, PAIRS)
        pltpu.make_async_copy(
            weight_ref.at[span], weights.at[span], weight_sem.at[part]
        ).wait()
        for i in range(PAIRS):
            pair = part * PAIRS + i
            product = lax.dot_general(
                areas[target_ref[pair]],
                weights[pair],
                (((1,), (1,)), ((), ())),
                preferred_element_type=jnp.float32,
            )
            row = product[0:8] + product[8:16]
            pair_rows[pl.ds(pair, 1), :] = row[0:1]
        return 0

    lax.fori_loop(0, pairs // PAIRS, part_of, 0)
    terms = three_terms(pair_rows[...])
    peer = lax.broadcasted_iota(jnp.int32, (PEERS, BLOCK), 0)
    capacity = blocks.shape[1]
    for slot in range(capacity):
        rows_of = jnp.zeros((PEERS, BLOCK), jnp.float32)
        for part in range(pairs // BLOCK):
            span = slice(part * BLOCK, (part + 1) * BLOCK)
            named = slot_ref[part : part + 1, :]
            chosen = jnp.where(peer * capacity + slot == named, 1.0, 0.0)
            chosen = chosen.astype(jnp.bfloat16)
            for term in terms:
                rows_of += jnp.dot(
                    chosen, term[span], preferred_element_type=jnp.float32
                )
        slot_rows[:, slot, :] = rows_of
    back[last] = slot_rows[me]
    for k in range(last):
        pltpu.make_async_remote_copy(
            src_ref=slot_rows.at[number(places[k])],
            dst_ref=back.at[opposite[k]],
            send_sem=back_send_sem,
            recv_sem=back_sem,
            device_id=places[k],
            device_id_type=MESH,
        ).start()
    for k in range(EARLY, MIDDLE):
        send(k)

    def source_part(part, total):
        columns = chunk(part, BLOCK)
        return total + source[:, columns].astype(jnp.float32) * area_ref[:, columns]

    zero = jnp.zeros((rows, BLOCK), jnp.float32)
    count = source.shape[1] // BLOCK
    source_total = lax.fori_loop(0, count, source_part, zero, unroll=8)
    most = pl.ds(0, last)
    pltpu.make_async_copy(slot_rows.at[most], back.at[most], back_sem).wait()

    def target_part(peer, total):
        for slot in range(capacity):
            factors = back[peer, pl.ds(slot, 1), :]
            total += blocks[peer, slot].astype(jnp.float32) * factors
        return total

    target_total = lax.fori_loop(0, PEERS, target_part, zero, unroll=4)
    column = jnp.concatenate(
        [
            jnp.sum(source_total, axis=1, keepdims=True),
            jnp.sum(target_total, axis=1, keepdims=True),
        ],
        axis=0,
    )
    own[...] = as_lanes(column)
    others[me] = own[...]
    for k in range(last):
        pltpu.make_async_remote_copy(
            src_ref=own,
            dst_ref=others.at[me],
            send_sem=mass_send_sem,
            recv_sem=mass_sem,
            device_id=places[k],
            device_id_type=MESH,
        ).start()
    for k in range(MIDDLE, last):
        send(k)
    pltpu.make_async_copy(others.at[most], others.at[most], mass_sem).wait()
    total = others[0]
    for k in range(1, PEERS):
        total += others[k]
    total_ref[...] = total
    pltpu.make_async_copy(others.at[most], others.at[most], mass_send_sem).wait()
    pltpu.make_async_copy(slot_rows.at[most], back.at[most], back_send_sem).wait()
    pltpu.make_async_copy(blocks.at[most], in_ref.at[most], send_sem).wait()
    pltpu.make_async_copy(blocks.at[most], in_ref.at[most], recv_sem).wait()


def exchanged(send_index, pair_slot, pair_target, target_area, area, source, weights):
    rows = source.shape[0]
    peers, capacity = send_index.shape[1:]
    targets = target_area.shape[0]
    pairs = weights.shape[0]
    blocks = (peers, capacity, rows, BLOCK)
    return pl.pallas_call(
        exchange,
        out_shape=(
            pltpu.VMEM(blocks, source.dtype),
            jax.ShapeDtypeStruct((1, 2 * rows), jnp.float32),
            pltpu.VMEM(weights.shape, weights.dtype),
        ),
        in_specs=[HBM] * 7,
        out_specs=(VMEM, VMEM, VMEM),
        scratch_shapes=[
            pltpu.SMEM((1, capacity, peers), jnp.int32),
            pltpu.SMEM((pairs,), jnp.int32),
            pltpu.VMEM((pairs // BLOCK, BLOCK), jnp.int32),
            pltpu.VMEM(target_area.shape, jnp.float32),
            pltpu.VMEM(area.shape, jnp.float32),
            pltpu.VMEM(source.shape, source.dtype),
            pltpu.VMEM(blocks, source.dtype),
            pltpu.VMEM((targets, 16, BLOCK), jnp.bfloat16),
            pltpu.VMEM((pairs, BLOCK), jnp.float32),
            pltpu.VMEM((peers, capacity, BLOCK), jnp.float32),
            pltpu.VMEM((peers, capacity, BLOCK), jnp.float32),
            pltpu.VMEM((1, 2 * rows), jnp.float32),
            pltpu.VMEM((peers, 1, 2 * rows), jnp.float32),
        ]
        + [pltpu.SemaphoreType.DMA] * 3
        + [pltpu.SemaphoreType.DMA((pairs // PAIRS,)), pltpu.SemaphoreType.DMA((5,))]
        + [pltpu.SemaphoreType.DMA] * 4,
        compiler_params=pltpu.CompilerParams(
            collective_id=1, has_side_effects=True, vmem_limit_bytes=EXCHANGE_VMEM
        ),
    )(
        *(
            pltpu.with_memory_space_constraint(operand, pltpu.HBM)
            for operand in (
                jnp.swapaxes(send_index, 1, 2),
                pair_target,
                pair_slot.reshape(-1, BLOCK),
                target_area,
                area,
                source,
                weights,
            )
        )
    )


def regrid(slot_ref, target_ref, total_ref, source_ref, weight_ref, out_ref):
    parts = weight_ref.shape[0] // PAIRS
    out_ref[...] = jnp.zeros_like(out_ref)

    def part_of(part, _):
        for i in range(PAIRS):
            pair = part * PAIRS + i
            product = jnp.dot(
                source_ref[slot_ref[pair]],
                weight_ref[pair],
                preferred_element_type=jnp.float32,
            )
            out_ref[:, chunk(target_ref[pair], BLOCK)] += product
        return 0

    lax.fori_loop(0, parts, part_of, 0)
    rows, cells = out_ref.shape
    total = jnp.transpose(jnp.broadcast_to(total_ref[...], (BLOCK, BLOCK)))
    scale = total[:rows] / total[rows : 2 * rows]
    for t in range(cells // BLOCK):
        columns = pl.ds(t * BLOCK, BLOCK)
        out_ref[:, columns] = out_ref[:, columns] * scale


def target_blocks(pair_slot, pair_target, inbound, weights, total, cells):
    rows = inbound.shape[1]
    return pl.pallas_call(
        regrid,
        out_shape=jax.ShapeDtypeStruct((rows, cells), jnp.float32),
        in_specs=[SMEM, SMEM, VMEM, VMEM, VMEM],
        out_specs=VMEM,
        compiler_params=pltpu.CompilerParams(vmem_limit_bytes=REGRID_VMEM),
    )(pair_slot, pair_target, total, inbound, weights)


def shards(src_field, src_area, tgt_area, weights, send_index, pair_slot, pair_target):
    rows = src_field.shape[0]
    peers, capacity = send_index.shape[1:]
    inbound, total, held = exchanged(
        send_index,
        pair_slot,
        pair_target,
        tgt_area.reshape(-1, BLOCK),
        src_area[None, :],
        src_field,
        weights,
    )
    inbound = inbound.reshape(peers * capacity, rows, BLOCK)
    return target_blocks(
        pair_slot, pair_target, inbound, held, total, tgt_area.shape[0]
    )


def solution(mesh):
    split = Mesh(mesh.devices.reshape(SIZES), AXES)
    placed = (
        P(None, AXES),
        P(AXES),
        P(AXES),
        P(AXES, None, None),
        P(AXES, None, None),
        P(AXES),
        P(AXES),
    )
    return jax.shard_map(
        shards, mesh=split, in_specs=placed, out_specs=P(None, AXES), check_vma=False
    )
```

```python
import itertools

import jax
import jax.numpy as jnp
from jax import lax
from jax.experimental import pallas as pl
from jax.experimental.pallas import tpu as pltpu
from jax.sharding import Mesh
from jax.sharding import PartitionSpec as P

AXES = ("z", "core", "y", "x")
SIZES = (4, 2, 4, 4)
PEERS = 128
BLOCK = 128
PAIRS = 32
PIECES = 4
EARLY = 32
MIDDLE = 64
EXCHANGE_VMEM = 36 * 1024 * 1024
REGRID_VMEM = 24 * 1024 * 1024
MESH = pl.DeviceIdType.MESH
ANY = pl.BlockSpec(memory_space=pl.ANY)
HBM = pl.BlockSpec(memory_space=pltpu.HBM)
SMEM = pl.BlockSpec(memory_space=pltpu.SMEM)
VMEM = pl.BlockSpec(memory_space=pltpu.VMEM)


def chunk(index, size):
    return pl.ds(pl.multiple_of(index * size, size), size)


def as_lanes(column):
    rows = column.shape[0]
    wide = jnp.broadcast_to(column, (rows, BLOCK))
    return jnp.transpose(wide)[0:1, :]


def routes():
    left = [offset for offset in itertools.product(*(range(size) for size in SIZES))][1:]

    def load(offset):
        links = [0] * 6
        for axis, step in enumerate((offset[0], offset[2], offset[3])):
            links[2 * axis] += step in (1, 2)
            links[2 * axis + 1] += step in (2, 3)
        return links

    used = [0] * 6
    order = []
    while left:
        def spread(offset):
            after = [a + b for a, b in zip(used, load(offset))]
            return max(after) - min(after)

        best = min(left, key=spread)
        left.remove(best)
        used = [a + b for a, b in zip(used, load(best))]
        order.append(best)
    return order


def three_terms(value):
    terms = []
    for _ in range(3):
        term = value.astype(jnp.bfloat16)
        terms.append(term)
        value = value - term.astype(jnp.float32)
    return terms


def exchange(
    index_hbm, target_hbm, slot_hbm, target_area_hbm, area_hbm, source_ref, weight_ref,
    in_ref, total_ref, weights,
    index_ref, target_ref, slot_ref, target_area_ref, area_ref,
    source, blocks, areas, pair_rows, slot_rows, back, own, others,
    send_sem, recv_sem, source_sem, weight_sem, small_sem,
    back_send_sem, back_sem, mass_send_sem, mass_sem,
):
    here = [lax.axis_index(axis) for axis in AXES]
    turned = [[lax.rem(h + k, size) for k in range(size)] for h, size in zip(here, SIZES)]
    offsets = routes()
    opposite = [
        offsets.index(tuple((-k) % size for k, size in zip(offset, SIZES)))
        for offset in offsets
    ]

    def number(place):
        value = place[0]
        for size, part in zip(SIZES[1:], place[1:]):
            value = value * size + part
        return value

    places = [tuple(axis[k] for axis, k in zip(turned, offset)) for offset in offsets]
    me = number(here)
    last = PEERS - 1
    rows = source.shape[0]
    pairs = weights.shape[0]
    barrier = pltpu.get_barrier_semaphore()
    far = pltpu.make_async_copy(source_ref, source, source_sem)
    far.start()
    small = [
        pltpu.make_async_copy(whole, held, small_sem.at[i])
        for i, (whole, held) in enumerate(
            (
                (index_hbm, index_ref),
                (target_hbm, target_ref),
                (slot_hbm, slot_ref),
                (target_area_hbm, target_area_ref),
                (area_hbm, area_ref),
            )
        )
    ]
    for copy in small:
        copy.start()
    for place in places:
        pl.semaphore_signal(barrier, inc=1, device_id=place, device_id_type=MESH)
    def gather(k):
        peer = me if k == last else number(places[k])
        for slot in range(blocks.shape[1]):
            block = jnp.maximum(index_ref[0, slot, peer], 0)
            blocks[k, slot] = source[:, pl.ds(block * BLOCK, BLOCK)]

    def send(k):
        pltpu.make_async_remote_copy(
            src_ref=blocks.at[k],
            dst_ref=in_ref.at[me],
            send_sem=send_sem,
            recv_sem=recv_sem,
            device_id=places[k],
            device_id_type=MESH,
        ).start()

    for copy in small:
        copy.wait()
    far.wait()
    for part in range(pairs // PAIRS):
        span = pl.ds(part * PAIRS, PAIRS)
        pltpu.make_async_copy(
            weight_ref.at[span], weights.at[span], weight_sem.at[part]
        ).start()
    for k in range(EARLY):
        gather(k)
    pl.semaphore_wait(barrier, PEERS - 1)
    for k in range(EARLY):
        send(k)
    for k in range(EARLY, PEERS):
        gather(k)
    in_ref[me] = blocks[last]

    area = target_area_ref[...]
    high = area.astype(jnp.bfloat16)
    low = (area - high.astype(jnp.float32)).astype(jnp.bfloat16)
    areas[:, 0:8, :] = jnp.broadcast_to(high[:, None, :], (area.shape[0], 8, BLOCK))
    areas[:, 8:16, :] = jnp.broadcast_to(low[:, None, :], (area.shape[0], 8, BLOCK))

    def part_of(part, _):
        span = chunk(part, PAIRS)
        pltpu.make_async_copy(
            weight_ref.at[span], weights.at[span], weight_sem.at[part]
        ).wait()
        for i in range(PAIRS):
            pair = part * PAIRS + i
            product = lax.dot_general(
                areas[target_ref[pair]],
                weights[pair],
                (((1,), (1,)), ((), ())),
                preferred_element_type=jnp.float32,
            )
            row = product[0:8] + product[8:16]
            pair_rows[pl.ds(pair, 1), :] = row[0:1]
        return 0

    lax.fori_loop(0, pairs // PAIRS, part_of, 0)
    terms = three_terms(pair_rows[...])
    peer = lax.broadcasted_iota(jnp.int32, (PEERS, BLOCK), 0)
    capacity = blocks.shape[1]
    for slot in range(capacity):
        rows_of = jnp.zeros((PEERS, BLOCK), jnp.float32)
        for part in range(pairs // BLOCK):
            span = slice(part * BLOCK, (part + 1) * BLOCK)
            named = slot_ref[part : part + 1, :]
            chosen = jnp.where(peer * capacity + slot == named, 1.0, 0.0)
            chosen = chosen.astype(jnp.bfloat16)
            for term in terms:
                rows_of += jnp.dot(
                    chosen, term[span], preferred_element_type=jnp.float32
                )
        slot_rows[:, slot, :] = rows_of
    back[last] = slot_rows[me]
    for k in range(last):
        pltpu.make_async_remote_copy(
            src_ref=slot_rows.at[number(places[k])],
            dst_ref=back.at[opposite[k]],
            send_sem=back_send_sem,
            recv_sem=back_sem,
            device_id=places[k],
            device_id_type=MESH,
        ).start()
    for k in range(EARLY, MIDDLE):
        send(k)

    def source_part(part, total):
        columns = chunk(part, BLOCK)
        return total + source[:, columns].astype(jnp.float32) * area_ref[:, columns]

    zero = jnp.zeros((rows, BLOCK), jnp.float32)
    count = source.shape[1] // BLOCK
    source_total = lax.fori_loop(0, count, source_part, zero, unroll=8)
    most = pl.ds(0, last)
    pltpu.make_async_copy(slot_rows.at[most], back.at[most], back_sem).wait()

    def target_part(peer, total):
        for slot in range(capacity):
            factors = back[peer, pl.ds(slot, 1), :]
            total += blocks[peer, slot].astype(jnp.float32) * factors
        return total

    target_total = lax.fori_loop(0, PEERS, target_part, zero, unroll=4)
    column = jnp.concatenate(
        [
            jnp.sum(source_total, axis=1, keepdims=True),
            jnp.sum(target_total, axis=1, keepdims=True),
        ],
        axis=0,
    )
    own[...] = as_lanes(column)
    others[me] = own[...]
    for k in range(last):
        pltpu.make_async_remote_copy(
            src_ref=own,
            dst_ref=others.at[me],
            send_sem=mass_send_sem,
            recv_sem=mass_sem,
            device_id=places[k],
            device_id_type=MESH,
        ).start()
    for k in range(MIDDLE, last):
        send(k)
    pltpu.make_async_copy(others.at[most], others.at[most], mass_sem).wait()
    total = others[0]
    for k in range(1, PEERS):
        total += others[k]
    total_ref[...] = total
    pltpu.make_async_copy(others.at[most], others.at[most], mass_send_sem).wait()
    pltpu.make_async_copy(slot_rows.at[most], back.at[most], back_send_sem).wait()
    pltpu.make_async_copy(blocks.at[most], in_ref.at[most], send_sem).wait()
    pltpu.make_async_copy(blocks.at[most], in_ref.at[most], recv_sem).wait()


def exchanged(send_index, pair_slot, pair_target, target_area, area, source, weights):
    rows = source.shape[0]
    peers, capacity = send_index.shape[1:]
    targets = target_area.shape[0]
    pairs = weights.shape[0]
    blocks = (peers, capacity, rows, BLOCK)
    return pl.pallas_call(
        exchange,
        out_shape=(
            pltpu.VMEM(blocks, source.dtype),
            jax.ShapeDtypeStruct((1, 2 * rows), jnp.float32),
            pltpu.VMEM(weights.shape, weights.dtype),
        ),
        in_specs=[HBM] * 7,
        out_specs=(VMEM, VMEM, VMEM),
        scratch_shapes=[
            pltpu.SMEM((1, capacity, peers), jnp.int32),
            pltpu.SMEM((pairs,), jnp.int32),
            pltpu.VMEM((pairs // BLOCK, BLOCK), jnp.int32),
            pltpu.VMEM(target_area.shape, jnp.float32),
            pltpu.VMEM(area.shape, jnp.float32),
            pltpu.VMEM(source.shape, source.dtype),
            pltpu.VMEM(blocks, source.dtype),
            pltpu.VMEM((targets, 16, BLOCK), jnp.bfloat16),
            pltpu.VMEM((pairs, BLOCK), jnp.float32),
            pltpu.VMEM((peers, capacity, BLOCK), jnp.float32),
            pltpu.VMEM((peers, capacity, BLOCK), jnp.float32),
            pltpu.VMEM((1, 2 * rows), jnp.float32),
            pltpu.VMEM((peers, 1, 2 * rows), jnp.float32),
        ]
        + [pltpu.SemaphoreType.DMA] * 3
        + [pltpu.SemaphoreType.DMA((pairs // PAIRS,)), pltpu.SemaphoreType.DMA((5,))]
        + [pltpu.SemaphoreType.DMA] * 4,
        compiler_params=pltpu.CompilerParams(
            collective_id=1, has_side_effects=True, vmem_limit_bytes=EXCHANGE_VMEM
        ),
    )(
        *(
            pltpu.with_memory_space_constraint(operand, pltpu.HBM)
            for operand in (
                jnp.swapaxes(send_index, 1, 2),
                pair_target,
                pair_slot.reshape(-1, BLOCK),
                target_area,
                area,
                source,
                weights,
            )
        )
    )


def regrid(
    slot_hbm, target_hbm, total_ref, source_ref, weight_ref, out_hbm,
    slot_ref, target_ref, out_ref, small_sem, out_sem,
):
    parts = weight_ref.shape[0] // PAIRS
    small = [
        pltpu.make_async_copy(slot_hbm, slot_ref, small_sem.at[0]),
        pltpu.make_async_copy(target_hbm, target_ref, small_sem.at[1]),
    ]
    for copy in small:
        copy.start()
    rows, cells = out_ref.shape
    total = jnp.transpose(jnp.broadcast_to(total_ref[...], (BLOCK, BLOCK)))
    scale = total[:rows] / total[rows : 2 * rows]
    out_ref[...] = jnp.zeros_like(out_ref)
    for copy in small:
        copy.wait()

    def part_of(part, _):
        for i in range(PAIRS):
            pair = part * PAIRS + i
            product = jnp.dot(
                source_ref[slot_ref[pair]],
                weight_ref[pair],
                preferred_element_type=jnp.float32,
            )
            out_ref[:, chunk(target_ref[pair], BLOCK)] += product
        return 0

    lax.fori_loop(0, parts, part_of, 0)
    width = cells // PIECES

    def leave(piece):
        columns = pl.ds(piece * width, width)
        return pltpu.make_async_copy(
            out_ref.at[:, columns], out_hbm.at[:, columns], out_sem.at[piece]
        )

    for piece in range(PIECES):
        for t in range(width // BLOCK):
            columns = pl.ds(piece * width + t * BLOCK, BLOCK)
            out_ref[:, columns] = out_ref[:, columns] * scale
        if piece > 0:
            leave(piece - 1).start()
    leave(PIECES - 1).start()
    for piece in range(PIECES):
        leave(piece).wait()


def target_blocks(pair_slot, pair_target, inbound, weights, total, cells):
    rows = inbound.shape[1]
    return pl.pallas_call(
        regrid,
        out_shape=jax.ShapeDtypeStruct((rows, cells), jnp.float32),
        in_specs=[HBM, HBM, VMEM, VMEM, VMEM],
        out_specs=ANY,
        scratch_shapes=[
            pltpu.SMEM(pair_slot.shape, jnp.int32),
            pltpu.SMEM(pair_target.shape, jnp.int32),
            pltpu.VMEM((rows, cells), jnp.float32),
            pltpu.SemaphoreType.DMA((2,)),
            pltpu.SemaphoreType.DMA((PIECES,)),
        ],
        compiler_params=pltpu.CompilerParams(vmem_limit_bytes=REGRID_VMEM),
    )(
        pltpu.with_memory_space_constraint(pair_slot, pltpu.HBM),
        pltpu.with_memory_space_constraint(pair_target, pltpu.HBM),
        total,
        inbound,
        weights,
    )


def shards(src_field, src_area, tgt_area, weights, send_index, pair_slot, pair_target):
    rows = src_field.shape[0]
    peers, capacity = send_index.shape[1:]
    inbound, total, held = exchanged(
        send_index,
        pair_slot,
        pair_target,
        tgt_area.reshape(-1, BLOCK),
        src_area[None, :],
        src_field,
        weights,
    )
    inbound = inbound.reshape(peers * capacity, rows, BLOCK)
    return target_blocks(
        pair_slot, pair_target, inbound, held, total, tgt_area.shape[0]
    )


def solution(mesh):
    split = Mesh(mesh.devices.reshape(SIZES), AXES)
    placed = (
        P(None, AXES),
        P(AXES),
        P(AXES),
        P(AXES, None, None),
        P(AXES, None, None),
        P(AXES),
        P(AXES),
    )
    return jax.shard_map(
        shards, mesh=split, in_specs=placed, out_specs=P(None, AXES), check_vma=False
    )
```

```python
import itertools

import jax
import jax.numpy as jnp
from jax import lax
from jax.experimental import pallas as pl
from jax.experimental.pallas import tpu as pltpu
from jax.sharding import Mesh
from jax.sharding import PartitionSpec as P

AXES = ("z", "core", "y", "x")
SIZES = (4, 2, 4, 4)
PEERS = 128
BLOCK = 128
PAIRS = 32
PIECES = 4
EARLY = 48
MIDDLE = 96
EXCHANGE_VMEM = 36 * 1024 * 1024
REGRID_VMEM = 24 * 1024 * 1024
MESH = pl.DeviceIdType.MESH
ANY = pl.BlockSpec(memory_space=pl.ANY)
HBM = pl.BlockSpec(memory_space=pltpu.HBM)
SMEM = pl.BlockSpec(memory_space=pltpu.SMEM)
VMEM = pl.BlockSpec(memory_space=pltpu.VMEM)


def chunk(index, size):
    return pl.ds(pl.multiple_of(index * size, size), size)


def as_lanes(column):
    rows = column.shape[0]
    wide = jnp.broadcast_to(column, (rows, BLOCK))
    return jnp.transpose(wide)[0:1, :]


def routes():
    left = [offset for offset in itertools.product(*(range(size) for size in SIZES))][1:]

    def load(offset):
        links = [0] * 6
        for axis, step in enumerate((offset[0], offset[2], offset[3])):
            links[2 * axis] += step in (1, 2)
            links[2 * axis + 1] += step in (2, 3)
        return links

    used = [0] * 6
    order = []
    while left:
        def spread(offset):
            after = [a + b for a, b in zip(used, load(offset))]
            return max(after) - min(after)

        best = min(left, key=spread)
        left.remove(best)
        used = [a + b for a, b in zip(used, load(best))]
        order.append(best)
    return order


def three_terms(value):
    terms = []
    for _ in range(3):
        term = value.astype(jnp.bfloat16)
        terms.append(term)
        value = value - term.astype(jnp.float32)
    return terms


def exchange(
    index_hbm, target_hbm, slot_hbm, target_area_hbm, area_hbm, source_ref, weight_ref,
    in_ref, total_ref, weights,
    index_ref, target_ref, slot_ref, target_area_ref, area_ref,
    source, blocks, areas, pair_rows, slot_rows, back, own, others,
    send_sem, recv_sem, source_sem, weight_sem, small_sem,
    back_send_sem, back_sem, mass_send_sem, mass_sem,
):
    here = [lax.axis_index(axis) for axis in AXES]
    turned = [[lax.rem(h + k, size) for k in range(size)] for h, size in zip(here, SIZES)]
    offsets = routes()
    opposite = [
        offsets.index(tuple((-k) % size for k, size in zip(offset, SIZES)))
        for offset in offsets
    ]

    def number(place):
        value = place[0]
        for size, part in zip(SIZES[1:], place[1:]):
            value = value * size + part
        return value

    places = [tuple(axis[k] for axis, k in zip(turned, offset)) for offset in offsets]
    me = number(here)
    last = PEERS - 1
    rows = source.shape[0]
    pairs = weights.shape[0]
    barrier = pltpu.get_barrier_semaphore()
    far = pltpu.make_async_copy(source_ref, source, source_sem)
    far.start()
    small = [
        pltpu.make_async_copy(whole, held, small_sem.at[i])
        for i, (whole, held) in enumerate(
            (
                (index_hbm, index_ref),
                (target_hbm, target_ref),
                (slot_hbm, slot_ref),
                (target_area_hbm, target_area_ref),
                (area_hbm, area_ref),
            )
        )
    ]
    for copy in small:
        copy.start()
    for place in places:
        pl.semaphore_signal(barrier, inc=1, device_id=place, device_id_type=MESH)
    def gather(k):
        peer = me if k == last else number(places[k])
        for slot in range(blocks.shape[1]):
            block = jnp.maximum(index_ref[0, slot, peer], 0)
            blocks[k, slot] = source[:, pl.ds(block * BLOCK, BLOCK)]

    def send(k):
        pltpu.make_async_remote_copy(
            src_ref=blocks.at[k],
            dst_ref=in_ref.at[me],
            send_sem=send_sem,
            recv_sem=recv_sem,
            device_id=places[k],
            device_id_type=MESH,
        ).start()

    for copy in small:
        copy.wait()
    far.wait()
    for part in range(pairs // PAIRS):
        span = pl.ds(part * PAIRS, PAIRS)
        pltpu.make_async_copy(
            weight_ref.at[span], weights.at[span], weight_sem.at[part]
        ).start()
    for k in range(EARLY):
        gather(k)
    pl.semaphore_wait(barrier, PEERS - 1)
    for k in range(EARLY):
        send(k)
    for k in range(EARLY, PEERS):
        gather(k)
    in_ref[me] = blocks[last]

    area = target_area_ref[...]
    high = area.astype(jnp.bfloat16)
    low = (area - high.astype(jnp.float32)).astype(jnp.bfloat16)
    areas[:, 0:8, :] = jnp.broadcast_to(high[:, None, :], (area.shape[0], 8, BLOCK))
    areas[:, 8:16, :] = jnp.broadcast_to(low[:, None, :], (area.shape[0], 8, BLOCK))

    def part_of(part, _):
        span = chunk(part, PAIRS)
        pltpu.make_async_copy(
            weight_ref.at[span], weights.at[span], weight_sem.at[part]
        ).wait()
        for i in range(PAIRS):
            pair = part * PAIRS + i
            product = lax.dot_general(
                areas[target_ref[pair]],
                weights[pair],
                (((1,), (1,)), ((), ())),
                preferred_element_type=jnp.float32,
            )
            row = product[0:8] + product[8:16]
            pair_rows[pl.ds(pair, 1), :] = row[0:1]
        return 0

    lax.fori_loop(0, pairs // PAIRS, part_of, 0)
    terms = three_terms(pair_rows[...])
    peer = lax.broadcasted_iota(jnp.int32, (PEERS, BLOCK), 0)
    capacity = blocks.shape[1]
    for slot in range(capacity):
        rows_of = jnp.zeros((PEERS, BLOCK), jnp.float32)
        for part in range(pairs // BLOCK):
            span = slice(part * BLOCK, (part + 1) * BLOCK)
            named = slot_ref[part : part + 1, :]
            chosen = jnp.where(peer * capacity + slot == named, 1.0, 0.0)
            chosen = chosen.astype(jnp.bfloat16)
            for term in terms:
                rows_of += jnp.dot(
                    chosen, term[span], preferred_element_type=jnp.float32
                )
        slot_rows[:, slot, :] = rows_of
    back[last] = slot_rows[me]
    for k in range(last):
        pltpu.make_async_remote_copy(
            src_ref=slot_rows.at[number(places[k])],
            dst_ref=back.at[opposite[k]],
            send_sem=back_send_sem,
            recv_sem=back_sem,
            device_id=places[k],
            device_id_type=MESH,
        ).start()
    for k in range(EARLY, MIDDLE):
        send(k)

    def source_part(part, total):
        columns = chunk(part, BLOCK)
        return total + source[:, columns].astype(jnp.float32) * area_ref[:, columns]

    zero = jnp.zeros((rows, BLOCK), jnp.float32)
    count = source.shape[1] // BLOCK
    source_total = lax.fori_loop(0, count, source_part, zero, unroll=8)
    most = pl.ds(0, last)
    pltpu.make_async_copy(slot_rows.at[most], back.at[most], back_sem).wait()

    def target_part(peer, total):
        for slot in range(capacity):
            factors = back[peer, pl.ds(slot, 1), :]
            total += blocks[peer, slot].astype(jnp.float32) * factors
        return total

    target_total = lax.fori_loop(0, PEERS, target_part, zero, unroll=4)
    column = jnp.concatenate(
        [
            jnp.sum(source_total, axis=1, keepdims=True),
            jnp.sum(target_total, axis=1, keepdims=True),
        ],
        axis=0,
    )
    own[...] = as_lanes(column)
    others[me] = own[...]
    for k in range(last):
        pltpu.make_async_remote_copy(
            src_ref=own,
            dst_ref=others.at[me],
            send_sem=mass_send_sem,
            recv_sem=mass_sem,
            device_id=places[k],
            device_id_type=MESH,
        ).start()
    for k in range(MIDDLE, last):
        send(k)
    pltpu.make_async_copy(others.at[most], others.at[most], mass_sem).wait()
    total = others[0]
    for k in range(1, PEERS):
        total += others[k]
    total_ref[...] = total
    pltpu.make_async_copy(others.at[most], others.at[most], mass_send_sem).wait()
    pltpu.make_async_copy(slot_rows.at[most], back.at[most], back_send_sem).wait()
    pltpu.make_async_copy(blocks.at[most], in_ref.at[most], send_sem).wait()
    pltpu.make_async_copy(blocks.at[most], in_ref.at[most], recv_sem).wait()


def exchanged(send_index, pair_slot, pair_target, target_area, area, source, weights):
    rows = source.shape[0]
    peers, capacity = send_index.shape[1:]
    targets = target_area.shape[0]
    pairs = weights.shape[0]
    blocks = (peers, capacity, rows, BLOCK)
    return pl.pallas_call(
        exchange,
        out_shape=(
            pltpu.VMEM(blocks, source.dtype),
            jax.ShapeDtypeStruct((1, 2 * rows), jnp.float32),
            pltpu.VMEM(weights.shape, weights.dtype),
        ),
        in_specs=[HBM] * 7,
        out_specs=(VMEM, VMEM, VMEM),
        scratch_shapes=[
            pltpu.SMEM((1, capacity, peers), jnp.int32),
            pltpu.SMEM((pairs,), jnp.int32),
            pltpu.VMEM((pairs // BLOCK, BLOCK), jnp.int32),
            pltpu.VMEM(target_area.shape, jnp.float32),
            pltpu.VMEM(area.shape, jnp.float32),
            pltpu.VMEM(source.shape, source.dtype),
            pltpu.VMEM(blocks, source.dtype),
            pltpu.VMEM((targets, 16, BLOCK), jnp.bfloat16),
            pltpu.VMEM((pairs, BLOCK), jnp.float32),
            pltpu.VMEM((peers, capacity, BLOCK), jnp.float32),
            pltpu.VMEM((peers, capacity, BLOCK), jnp.float32),
            pltpu.VMEM((1, 2 * rows), jnp.float32),
            pltpu.VMEM((peers, 1, 2 * rows), jnp.float32),
        ]
        + [pltpu.SemaphoreType.DMA] * 3
        + [pltpu.SemaphoreType.DMA((pairs // PAIRS,)), pltpu.SemaphoreType.DMA((5,))]
        + [pltpu.SemaphoreType.DMA] * 4,
        compiler_params=pltpu.CompilerParams(
            collective_id=1, has_side_effects=True, vmem_limit_bytes=EXCHANGE_VMEM
        ),
    )(
        *(
            pltpu.with_memory_space_constraint(operand, pltpu.HBM)
            for operand in (
                jnp.swapaxes(send_index, 1, 2),
                pair_target,
                pair_slot.reshape(-1, BLOCK),
                target_area,
                area,
                source,
                weights,
            )
        )
    )


def regrid(
    slot_hbm, target_hbm, total_ref, source_ref, weight_ref, out_hbm,
    slot_ref, target_ref, out_ref, small_sem, out_sem,
):
    parts = weight_ref.shape[0] // PAIRS
    small = [
        pltpu.make_async_copy(slot_hbm, slot_ref, small_sem.at[0]),
        pltpu.make_async_copy(target_hbm, target_ref, small_sem.at[1]),
    ]
    for copy in small:
        copy.start()
    rows, cells = out_ref.shape
    total = jnp.transpose(jnp.broadcast_to(total_ref[...], (BLOCK, BLOCK)))
    scale = total[:rows] / total[rows : 2 * rows]
    out_ref[...] = jnp.zeros_like(out_ref)
    for copy in small:
        copy.wait()

    def part_of(part, _):
        for i in range(PAIRS):
            pair = part * PAIRS + i
            product = jnp.dot(
                source_ref[slot_ref[pair]],
                weight_ref[pair],
                preferred_element_type=jnp.float32,
            )
            out_ref[:, chunk(target_ref[pair], BLOCK)] += product
        return 0

    lax.fori_loop(0, parts, part_of, 0)
    width = cells // PIECES

    def leave(piece):
        columns = pl.ds(piece * width, width)
        return pltpu.make_async_copy(
            out_ref.at[:, columns], out_hbm.at[:, columns], out_sem.at[piece]
        )

    for piece in range(PIECES):
        for t in range(width // BLOCK):
            columns = pl.ds(piece * width + t * BLOCK, BLOCK)
            out_ref[:, columns] = out_ref[:, columns] * scale
        if piece > 0:
            leave(piece - 1).start()
    leave(PIECES - 1).start()
    for piece in range(PIECES):
        leave(piece).wait()


def target_blocks(pair_slot, pair_target, inbound, weights, total, cells):
    rows = inbound.shape[1]
    return pl.pallas_call(
        regrid,
        out_shape=jax.ShapeDtypeStruct((rows, cells), jnp.float32),
        in_specs=[HBM, HBM, VMEM, VMEM, VMEM],
        out_specs=ANY,
        scratch_shapes=[
            pltpu.SMEM(pair_slot.shape, jnp.int32),
            pltpu.SMEM(pair_target.shape, jnp.int32),
            pltpu.VMEM((rows, cells), jnp.float32),
            pltpu.SemaphoreType.DMA((2,)),
            pltpu.SemaphoreType.DMA((PIECES,)),
        ],
        compiler_params=pltpu.CompilerParams(vmem_limit_bytes=REGRID_VMEM),
    )(
        pltpu.with_memory_space_constraint(pair_slot, pltpu.HBM),
        pltpu.with_memory_space_constraint(pair_target, pltpu.HBM),
        total,
        inbound,
        weights,
    )


def shards(src_field, src_area, tgt_area, weights, send_index, pair_slot, pair_target):
    rows = src_field.shape[0]
    peers, capacity = send_index.shape[1:]
    inbound, total, held = exchanged(
        send_index,
        pair_slot,
        pair_target,
        tgt_area.reshape(-1, BLOCK),
        src_area[None, :],
        src_field,
        weights,
    )
    inbound = inbound.reshape(peers * capacity, rows, BLOCK)
    return target_blocks(
        pair_slot, pair_target, inbound, held, total, tgt_area.shape[0]
    )


def solution(mesh):
    split = Mesh(mesh.devices.reshape(SIZES), AXES)
    placed = (
        P(None, AXES),
        P(AXES),
        P(AXES),
        P(AXES, None, None),
        P(AXES, None, None),
        P(AXES),
        P(AXES),
    )
    return jax.shard_map(
        shards, mesh=split, in_specs=placed, out_specs=P(None, AXES), check_vma=False
    )
```
